128 devices in a mesh: row: 8 (over x_lo, z), col: 16 (over x_hi, y, core).
Axes of the slice: x: 4 (x_hi: 2, x_lo: 2; x = x_hi * 2 + x_lo), y: 4, z: 4, core: 2. Of those that a mesh axis runs over, the one named last changes fastest.
Arguments:
- loadings: float32 [64, 32, 16384], P(None, None, ('row', 'col')), may hold values from -6 to 6
Outputs:
- correlation: float32 [16384, 16384], P('row', 'col')
The draws below stay inside these ranges and needn't reach their ends.
All inputs are finite; a program needn't handle non-finite values.
Results may differ from the reference program's by a relative error of at most 0.000096.
Values sent between devices are 32-bit elements; how exact they have to be, the bound alone decides.
A program may use at most 128 MiB of HBM per device.

```python
import jax
import jax.numpy as jnp
from jax import lax

SPECIES = 16384
FACTORS = 32
SAMPLES = 64


def shard_levels(own_key, extent, split, low, top_value):
    def one(axis_at, blocks):
        draws = jax.random.uniform(jax.random.fold_in(jax.random.fold_in(own_key, 6), axis_at), (blocks,), jnp.float32, low / len(split), top_value / len(split))
        return jnp.repeat(jnp.exp(draws), extent[axis_at] // blocks).reshape((-1,) + (1,) * (len(extent) - axis_at - 1))

    factor_of = one(*split[0])
    for cut in split[1:]:
        factor_of = factor_of * one(*cut)
    return factor_of


def gaussian(key, dims, width, most, pieces=(), held_as=jnp.bfloat16):
    factor_of = shard_levels(key, dims, pieces, -0.22, 0.18) if pieces else 1.0
    array = jax.random.normal(key, dims, jnp.float32) * width * factor_of
    return jnp.minimum(jnp.maximum(array, -most), most).astype(held_as)


def setup_inputs(seed: int = 0) -> dict:
    streams_of = jax.random.split(jax.random.key(seed), 2)
    return {
        "loadings": gaussian(streams_of[0], (SAMPLES, FACTORS, SPECIES), 1.0, 6.0, ((2, 128),), jnp.float32),
    }


def reference(loadings):
    variance = lax.optimization_barrier(jnp.sum(loadings * loadings, axis=1, keepdims=True))
    scaled = loadings / jnp.sqrt(variance)
    flat = scaled.reshape(SAMPLES * FACTORS, SPECIES)
    total = jnp.dot(flat.T, flat, precision=lax.Precision.HIGHEST, preferred_element_type=jnp.float32)
    return total * (1.0 / SAMPLES)
```

```python
import functools

import jax
import jax.numpy as jnp
from jax import lax
from jax.experimental import pallas as pl
from jax.experimental.pallas import tpu as pltpu
from jax.sharding import PartitionSpec as P

MESH = pl.DeviceIdType.MESH
SAMPLES, FACTORS, BLOCK = 64, 32, 128
DEPTH = SAMPLES * FACTORS
PIECES = 8
ROWS = BLOCK // PIECES
DEEP = DEPTH // PIECES
PAIR = 2 * BLOCK


def place(a, b, y, z, c):
    return (b * 4 + z, a * 8 + y * 2 + c)


def kernel(
    x_ref,
    out_ref,
    rbuf,
    cbuf,
    csend,
    rhi,
    rlo,
    chi,
    clo,
    outbuf,
    send,
    t_recv,
    x_recv,
    b_recv,
    y1_recv,
    y2_recv,
    z1_recv,
    z2_recv,
    d_recv,
    out_sem,
):
    row, col = lax.axis_index("row"), lax.axis_index("col")
    b, z = row // 4, row % 4
    a, y, c = col // 8, (col // 2) % 4, col % 2
    up, down = 1, 3

    twin = place(a, b, y, z, 1 - c)
    across = place(1 - a, b, y, z, c)
    beside = place(a, 1 - b, y, z, c)
    y_dev = {d: place(a, b, (y + d) % 4, z, c) for d in (up, down)}
    z_dev = {d: place(a, b, y, (z + d) % 4, c) for d in (up, down)}
    t_to = place(b, 1 - c, z, (2 * z + 4 - y) % 4, a)
    t_from = place(c, a, (2 * y + 4 - z) % 4, y, 1 - b)

    def r_pair(flip, dy):
        return (a + flip) % 2 * 4 + (y + dy) % 4

    def c_pair(dz):
        return (2 * y + 8 - z - dz) % 4

    barrier = pltpu.get_barrier_semaphore()
    for device in (twin, across, beside, y_dev[up], y_dev[down], z_dev[up], z_dev[down], t_from):
        pl.semaphore_signal(barrier, inc=1, device_id=device, device_id_type=MESH)

    own = r_pair(0, 0) * 2 + c

    def normalise(i, _):
        x = x_ref[pl.ds(i * 8, 8)]
        variance = jnp.sum(x * x, axis=1, keepdims=True)
        scaled = (x * (1.0 / jnp.sqrt(variance))).reshape(8 * FACTORS, BLOCK)
        at = pl.ds(pl.multiple_of(i * 8 * FACTORS, 8 * FACTORS), 8 * FACTORS)
        csend[at, :] = scaled
        rbuf[own, :, at] = scaled.T
        return 0

    lax.fori_loop(0, SAMPLES // 8, normalise, 0)
    pl.semaphore_wait(barrier, 8)

    def go(src, dst, sem, recv, device):
        pltpu.make_async_remote_copy(
            src_ref=src, dst_ref=dst, send_sem=send.at[sem], recv_sem=recv, device_id=device, device_id_type=MESH
        ).start()

    def r_piece(block, i):
        return rbuf.at[block, pl.ds(i * ROWS, ROWS), :]

    def c_piece(block, i):
        return cbuf.at[block, pl.ds(i * DEEP, DEEP), :]

    def arrived(ref, sem):
        pltpu.make_async_copy(ref, ref, sem).wait()

    def r_go(block, i, sem, recv, device):
        go(r_piece(block, i), r_piece(block, i), sem, recv, device)

    def c_go(block, i, sem, recv, device):
        go(c_piece(block, i), c_piece(block, i), sem, recv, device)

    S_T, S_X, S_B, S_YU, S_YD, S_ZU, S_ZD, S_D = range(8)

    def hand_over(flip, dy):
        pair = r_pair(flip, dy)
        go(rbuf.at[pair * 2 + c], rbuf.at[pair * 2 + c], S_D, d_recv.at[pair], twin)

    def y_first(k, i):
        block = r_pair(k, 0) * 2 + c
        r_go(block, i, S_YU, y1_recv.at[0, k, i], y_dev[up])
        r_go(block, i, S_YD, y1_recv.at[1, k, i], y_dev[down])

    def z_first(k, block, i):
        c_go(block, i, S_ZU, z1_recv.at[0, k, i], z_dev[up])
        c_go(block, i, S_ZD, z1_recv.at[1, k, i], z_dev[down])

    def each(n, body):
        def step(i, _):
            body(i)
            return 0

        lax.fori_loop(0, n, step, 0)

    t_slot = y * 2 + c
    own_t = c_pair(0) * 2 + 1 - b
    own_b = c_pair(0) * 2 + b

    def start(i):
        go(csend.at[pl.ds(i * DEEP, DEEP), :], c_piece(t_slot, i), S_T, t_recv.at[i], t_to)
        r_go(own, i, S_X, x_recv.at[i], across)
        y_first(0, i)

    each(PIECES, start)
    hand_over(0, 0)

    def split_rows(pair, half):
        def body(i):
            at = pl.ds(pl.multiple_of(i * 16, 16), 16)
            v = rbuf[pair * 2 + half, at, :]
            hi = v.astype(jnp.bfloat16)
            to = pl.ds(pl.multiple_of(half * BLOCK + i * 16, 16), 16)
            rhi[pair, to, :] = hi
            rlo[pair, to, :] = (v - hi.astype(jnp.float32)).astype(jnp.bfloat16)

        each(BLOCK // 16, body)

    def ready_rows(flip, dy):
        pair = r_pair(flip, dy)
        arrived(rbuf.at[pair * 2 + 1 - c], d_recv.at[pair])
        split_rows(pair, 0)
        split_rows(pair, 1)

    def ready_columns(dz):
        pair = c_pair(dz)

        def body(i):
            at = pl.ds(pl.multiple_of(i * DEEP, DEEP), DEEP)
            for half in range(2):
                v = cbuf[pair * 2 + half, at, :]
                hi = v.astype(jnp.bfloat16)
                to = slice(half * BLOCK, (half + 1) * BLOCK)
                chi[pair, at, to] = hi
                clo[pair, at, to] = (v - hi.astype(jnp.float32)).astype(jnp.bfloat16)

        each(PIECES, body)

    def dot(left, right):
        return jnp.dot(left, right, preferred_element_type=jnp.float32)

    def tile(p, q):
        total = dot(rhi[p], chi[q]) + dot(rhi[p], clo[q]) + dot(rlo[p], chi[q])
        rows = pl.ds(pl.multiple_of(p * PAIR, PAIR), PAIR)
        columns = pl.ds(pl.multiple_of(q * PAIR, PAIR), PAIR)
        outbuf[rows, columns] = total * (1.0 / SAMPLES)
        pltpu.make_async_copy(outbuf.at[rows, columns], out_ref.at[rows, columns], out_sem).start()

    def turn(m):
        return m + m // 2 - 2 * (m // 3)

    ready_rows(0, 0)

    def relay(i):
        arrived(c_piece(own_t, i), t_recv.at[i])
        z_first(0, own_t, i)
        c_go(own_t, i, S_B, b_recv.at[i], beside)
        arrived(r_piece(r_pair(1, 0) * 2 + c, i), x_recv.at[i])
        y_first(1, i)

        @pl.when(i > 0)
        def _():
            arrived(c_piece(own_b, i - 1), b_recv.at[i - 1])
            z_first(1, own_b, i - 1)

    each(PIECES, relay)
    arrived(c_piece(own_b, PIECES - 1), b_recv.at[PIECES - 1])
    z_first(1, own_b, PIECES - 1)
    hand_over(1, 0)

    def y_second(k, half):
        even, odd = 2 * half, 2 * half + 1
        below, above = r_pair(k, down) * 2 + c, r_pair(k, up) * 2 + c
        for i in (even, odd):
            arrived(r_piece(below, i), y1_recv.at[0, k, i])
            arrived(r_piece(above, i), y1_recv.at[1, k, i])
        r_go(below, even, S_YU, y2_recv.at[0, k, half], y_dev[up])
        r_go(above, odd, S_YD, y2_recv.at[1, k, half], y_dev[down])

    def z_second(half):
        even, odd = 2 * half, 2 * half + 1
        for k in range(2):
            s = (1 - b + k) % 2
            below, above = c_pair(down) * 2 + s, c_pair(up) * 2 + s
            for i in (even, odd):
                arrived(c_piece(below, i), z1_recv.at[0, k, i])
                arrived(c_piece(above, i), z1_recv.at[1, k, i])
            c_go(below, even, S_ZU, z2_recv.at[0, k, half], z_dev[up])
            c_go(above, odd, S_ZD, z2_recv.at[1, k, half], z_dev[down])

    each(PIECES // 2, lambda half: y_second(0, half))
    hand_over(0, up)
    hand_over(0, down)
    ready_rows(1, 0)
    ready_columns(0)
    each(2, lambda k: tile(r_pair(k, 0), c_pair(0)))
    ready_rows(0, up)
    ready_rows(0, down)
    each(2, lambda k: tile(r_pair(0, 1 + 2 * k), c_pair(0)))

    def second(half):
        z_second(half)
        y_second(1, half)

    each(PIECES // 2, second)
    hand_over(1, up)
    hand_over(1, down)
    ready_columns(up)
    ready_columns(down)
    ready_rows(1, up)
    ready_rows(1, down)
    each(2, lambda k: tile(r_pair(1, 1 + 2 * k), c_pair(0)))
    each(12, lambda k: tile(r_pair(k % 2, turn(k // 2 % 3)), c_pair(1 + 2 * (k // 6))))

    def y_last(k):
        far = r_pair(k, 2) * 2 + c
        for half in range(PIECES // 2):
            arrived(r_piece(far, 2 * half), y2_recv.at[0, k, half])
            arrived(r_piece(far, 2 * half + 1), y2_recv.at[1, k, half])
        hand_over(k, 2)

    for k in range(2):
        y_last(k)
        ready_rows(k, 2)
        each(3, lambda m: tile(r_pair(k, 2), c_pair(turn(m))))

    for k in range(2):
        far = c_pair(2) * 2 + (1 - b + k) % 2
        for half in range(PIECES // 2):
            arrived(c_piece(far, 2 * half), z2_recv.at[0, k, half])
            arrived(c_piece(far, 2 * half + 1), z2_recv.at[1, k, half])
    ready_columns(2)
    each(8, lambda k: tile(k, c_pair(2)))

    for sem, blocks in ((S_T, 1), (S_X, 1), (S_B, 1), (S_YU, 3), (S_YD, 3), (S_ZU, 3), (S_ZD, 3), (S_D, 8)):
        arrived(rbuf.at[pl.ds(0, blocks)], send.at[sem])
    pltpu.make_async_copy(outbuf, out_ref, out_sem).wait()


def local(loadings):
    dma = pltpu.SemaphoreType.DMA
    return pl.pallas_call(
        kernel,
        out_shape=jax.ShapeDtypeStruct((16 * BLOCK, 8 * BLOCK), jnp.float32),
        in_specs=[pl.BlockSpec(memory_space=pltpu.VMEM)],
        out_specs=pl.BlockSpec(memory_space=pl.ANY),
        scratch_shapes=[
            pltpu.VMEM((16, BLOCK, DEPTH), jnp.float32),
            pltpu.VMEM((8, DEPTH, BLOCK), jnp.float32),
            pltpu.VMEM((DEPTH, BLOCK), jnp.float32),
            pltpu.VMEM((8, PAIR, DEPTH), jnp.bfloat16),
            pltpu.VMEM((8, PAIR, DEPTH), jnp.bfloat16),
            pltpu.VMEM((4, DEPTH, PAIR), jnp.bfloat16),
            pltpu.VMEM((4, DEPTH, PAIR), jnp.bfloat16),
            pltpu.VMEM((16 * BLOCK, 8 * BLOCK), jnp.float32),
            dma((8,)),
            dma((PIECES,)),
            dma((PIECES,)),
            dma((PIECES,)),
            dma((2, 2, PIECES)),
            dma((2, 2, PIECES // 2)),
            dma((2, 2, PIECES)),
            dma((2, 2, PIECES // 2)),
            dma((8,)),
            dma,
        ],
        compiler_params=pltpu.CompilerParams(
            collective_id=0, has_side_effects=True, vmem_limit_bytes=61 * 1024 * 1024
        ),
    )(loadings)


def solution(mesh):
    placed = (P(None, None, ("row", "col")),)
    return jax.shard_map(local, mesh=mesh, in_specs=placed, out_specs=P("row", "col"), check_vma=False)
```

```python
import functools

import jax
import jax.numpy as jnp
from jax import lax
from jax.experimental import pallas as pl
from jax.experimental.pallas import tpu as pltpu
from jax.sharding import PartitionSpec as P

MESH = pl.DeviceIdType.MESH
SAMPLES, FACTORS, BLOCK = 64, 32, 128
DEPTH = SAMPLES * FACTORS
PIECES = 8
ROWS = BLOCK // PIECES
DEEP = DEPTH // PIECES
PAIR = 2 * BLOCK


def place(a, b, y, z, c):
    return (b * 4 + z, a * 8 + y * 2 + c)


def kernel(
    x_ref,
    out_ref,
    rbuf,
    cbuf,
    csend,
    tbuf,
    rhi,
    rlo,
    chi,
    clo,
    outbuf,
    send,
    t_recv,
    tr_recv,
    x_recv,
    b_recv,
    y1_recv,
    y2_recv,
    z1_recv,
    z2_recv,
    d_recv,
    out_sem,
):
    row, col = lax.axis_index("row"), lax.axis_index("col")
    b, z = row // 4, row % 4
    a, y, c = col // 8, (col // 2) % 4, col % 2
    up, down = 1, 3

    twin = place(a, b, y, z, 1 - c)
    across = place(1 - a, b, y, z, c)
    beside = place(a, 1 - b, y, z, c)
    y_dev = {d: place(a, b, (y + d) % 4, z, c) for d in (up, down)}
    z_dev = {d: place(a, b, y, (z + d) % 4, c) for d in (up, down)}
    t_to = place(b, 1 - c, z, (2 * z + 4 - y) % 4, a)
    t_from = place(c, a, (2 * y + 4 - z) % 4, y, 1 - b)
    off = (y + 4 - z) % 4
    turns = (1, 3)

    def corner_from(e):
        return place(c, a, (y + 6 - e) % 4, (z + 4 - e) % 4, 1 - b)

    def corner_to(e):
        return place(a, b, (y + 4 - e) % 4, (z + 6 - e) % 4, c)

    def side_from(d):
        return place(c, a, y, (y + 4 - d) % 4, 1 - b)

    def side_to(d):
        return place(a, b, (y + 4 - d) % 4, z, c)

    def r_pair(flip, dy):
        return (a + flip) % 2 * 4 + (y + dy) % 4

    def c_pair(dz):
        return (2 * y + 8 - z - dz) % 4

    barrier = pltpu.get_barrier_semaphore()

    def here(*devices):
        for device in devices:
            pl.semaphore_signal(barrier, inc=1, device_id=device, device_id_type=MESH)

    here(twin, across, beside, y_dev[up], y_dev[down], z_dev[up], z_dev[down], t_from)

    @pl.when(off % 2 == 1)
    def _():
        here(place(a, b, (y + off) % 4, z, c))

    @pl.when(off == 2)
    def _():
        here(*(side_from(d) for d in turns))
        here(*(place(a, b, (y + e) % 4, (y + e) % 4, c) for e in turns))

    @pl.when(off == 0)
    def _():
        here(*(corner_from(e) for e in turns))

    own = r_pair(0, 0) * 2 + c

    def normalise(i, _):
        x = x_ref[pl.ds(i * 8, 8)]
        variance = jnp.sum(x * x, axis=1, keepdims=True)
        scaled = (x * (1.0 / jnp.sqrt(variance))).reshape(8 * FACTORS, BLOCK)
        at = pl.ds(pl.multiple_of(i * 8 * FACTORS, 8 * FACTORS), 8 * FACTORS)
        csend[at, :] = scaled
        rbuf[own, :, at] = scaled.T
        return 0

    lax.fori_loop(0, SAMPLES // 8, normalise, 0)
    odd = off % 2
    pl.semaphore_wait(barrier, 8 + odd + (1 - odd) * (2 + 2 * (off // 2)))

    def go(src, dst, sem, recv, device):
        pltpu.make_async_remote_copy(
            src_ref=src, dst_ref=dst, send_sem=send.at[sem], recv_sem=recv, device_id=device, device_id_type=MESH
        ).start()

    def r_piece(block, i):
        return rbuf.at[block, pl.ds(i * ROWS, ROWS), :]

    def c_piece(block, i):
        return cbuf.at[block, pl.ds(i * DEEP, DEEP), :]

    def arrived(ref, sem):
        pltpu.make_async_copy(ref, ref, sem).wait()

    def r_go(block, i, sem, recv, device):
        go(r_piece(block, i), r_piece(block, i), sem, recv, device)

    def c_go(block, i, sem, recv, device):
        go(c_piece(block, i), c_piece(block, i), sem, recv, device)

    S_T, S_X, S_B, S_YU, S_YD, S_ZU, S_ZD, S_D, S_TR = range(9)

    def hand_over(flip, dy):
        pair = r_pair(flip, dy)
        go(rbuf.at[pair * 2 + c], rbuf.at[pair * 2 + c], S_D, d_recv.at[pair], twin)

    def y_first(k, i):
        block = r_pair(k, 0) * 2 + c
        r_go(block, i, S_YU, y1_recv.at[0, k, i], y_dev[up])
        r_go(block, i, S_YD, y1_recv.at[1, k, i], y_dev[down])

    def z_first(k, block, i):
        c_go(block, i, S_ZU, z1_recv.at[0, k, i], z_dev[up])
        c_go(block, i, S_ZD, z1_recv.at[1, k, i], z_dev[down])

    def each(n, body):
        def step(i, _):
            body(i)
            return 0

        lax.fori_loop(0, n, step, 0)

    t_slot = y * 2 + c
    own_t = c_pair(0) * 2 + 1 - b
    own_b = c_pair(0) * 2 + b

    def transposed(i):
        src = csend.at[pl.ds(i * DEEP, DEEP), :]
        aside = (off % 2) * (i % 4 // 3) + (off // 2) * (1 - off % 2)
        f, slot = i % 2, i // 2

        @pl.when(aside == 0)
        def _():
            go(src, c_piece(t_slot, i), S_T, t_recv.at[i], t_to)

        @pl.when(aside * (off % 2) == 1)
        def _():
            g = off // 2
            go(src, tbuf.at[g, i // 4], S_T, tr_recv.at[g, i // 4], place(b, 1 - c, y, (z + 4 - off) % 4, a))

        @pl.when(aside * (1 - off % 2) == 1)
        def _():
            w = (z + 1 + 2 * f) % 4
            go(src, tbuf.at[f, slot], S_T, tr_recv.at[f, slot], place(b, 1 - c, w, w, a))

    def start(i):
        y_first(0, i)

    def pass_corner(i):
        f, slot = i % 2, i // 2

        @pl.when(off == 0)
        def _():
            e = 1 + 2 * f
            arrived(tbuf.at[f, slot], tr_recv.at[f, slot])
            at = (y + 6 - e) % 4 * 2 + 1 - b
            go(tbuf.at[f, slot], c_piece(at, i), S_TR, t_recv.at[i], corner_to(e))

    def pass_side(i):
        f, slot = i % 2, i // 2

        @pl.when((off // 2) * (1 - off % 2) * (1 - i // 4) == 1)
        def _():
            arrived(tbuf.at[f, slot], tr_recv.at[f, slot])
            p = 4 * slot + 3
            go(tbuf.at[f, slot], c_piece(y * 2 + 1 - b, p), S_TR, t_recv.at[p], side_to(1 + 2 * f))

    each(PIECES, transposed)
    each(PIECES, start)
    hand_over(0, 0)

    def split_rows(pair, half):
        def body(i):
            at = pl.ds(pl.multiple_of(i * 16, 16), 16)
            v = rbuf[pair * 2 + half, at, :]
            hi = v.astype(jnp.bfloat16)
            to = pl.ds(pl.multiple_of(pair * PAIR + half * BLOCK + i * 16, 16), 16)
            rhi[to, :] = hi
            rlo[to, :] = (v - hi.astype(jnp.float32)).astype(jnp.bfloat16)

        each(BLOCK // 16, body)

    def ready_rows(flip, dy):
        pair = r_pair(flip, dy)
        arrived(rbuf.at[pair * 2 + 1 - c], d_recv.at[pair])
        split_rows(pair, 0)
        split_rows(pair, 1)

    def blocks_of(slot):
        beyond = (slot + 1) // 2
        which = (slot + b) % 2
        left = (1 - beyond) * (c_pair(0) * 2) + beyond * (c_pair(up) * 2 + which)
        right = (1 - beyond) * (c_pair(0) * 2 + 1) + beyond * (c_pair(down) * 2 + which)
        return left, right

    def ready_columns(slot):
        for side, block in enumerate(blocks_of(slot)):

            def body(i):
                at = pl.ds(pl.multiple_of(i * DEEP, DEEP), DEEP)
                v = cbuf[block, at, :]
                hi = v.astype(jnp.bfloat16)
                to = slice(side * BLOCK, (side + 1) * BLOCK)
                chi[slot, at, to] = hi
                clo[slot, at, to] = (v - hi.astype(jnp.float32)).astype(jnp.bfloat16)

            each(PIECES, body)

    def dot(left, right):
        return jnp.dot(left, right, preferred_element_type=jnp.float32)

    def tile(p, slot):
        rows = pl.ds(pl.multiple_of(p * PAIR, PAIR), PAIR)
        right = chi[slot]
        total = dot(rhi[rows, :], right) + dot(rhi[rows, :], clo[slot]) + dot(rlo[rows, :], right)
        total = total * (1.0 / SAMPLES)
        for side, block in enumerate(blocks_of(slot)):
            columns = pl.ds(pl.multiple_of(block * BLOCK, BLOCK), BLOCK)
            outbuf[rows, columns] = total[:, side * BLOCK : (side + 1) * BLOCK]
            pltpu.make_async_copy(outbuf.at[rows, columns], out_ref.at[rows, columns], out_sem).start()

    def turn(m):
        return m + m // 2 - 2 * (m // 3)

    ready_rows(0, 0)

    def y_second(k, half):
        even, odd = 2 * half, 2 * half + 1
        below, above = r_pair(k, down) * 2 + c, r_pair(k, up) * 2 + c
        for i in (even, odd):
            arrived(r_piece(below, i), y1_recv.at[0, k, i])
            arrived(r_piece(above, i), y1_recv.at[1, k, i])
        r_go(below, even, S_YU, y2_recv.at[0, k, half], y_dev[up])
        r_go(above, odd, S_YD, y2_recv.at[1, k, half], y_dev[down])

    def z_second(k, half):
        even, odd = 2 * half, 2 * half + 1
        s = (1 - b + k) % 2
        below, above = c_pair(down) * 2 + s, c_pair(up) * 2 + s
        for i in (even, odd):
            arrived(c_piece(below, i), z1_recv.at[0, k, i])
            arrived(c_piece(above, i), z1_recv.at[1, k, i])
        c_go(below, even, S_ZU, z2_recv.at[0, k, half], z_dev[up])
        c_go(above, odd, S_ZD, z2_recv.at[1, k, half], z_dev[down])

    def early(i):
        @pl.when((off // 2) * (1 - off % 2) * (i % 2) == 1)
        def _():
            z_second(0, i // 2)

        pass_side(i)
        arrived(c_piece(own_t, i), t_recv.at[i])
        z_first(0, own_t, i)
        c_go(own_t, i, S_B, b_recv.at[i], beside)
        r_go(own, i, S_X, x_recv.at[i], across)
        pass_corner(i)

        @pl.when(i >= PIECES // 2)
        def _():
            y_second(0, i - PIECES // 2)

            @pl.when(off == 0)
            def _():
                z_second(0, i - PIECES // 2)

    each(PIECES, early)

    def middle(i):
        arrived(r_piece(r_pair(1, 0) * 2 + c, i), x_recv.at[i])
        y_first(1, i)

        @pl.when((i % 2) * (off % 2) == 1)
        def _():
            z_second(0, i // 2)

        arrived(c_piece(own_b, i), b_recv.at[i])
        z_first(1, own_b, i)

    each(PIECES, middle)
    hand_over(0, up)
    hand_over(0, down)
    hand_over(1, 0)
    ready_columns(0)
    ready_columns(1)

    def y_last(k):
        far = r_pair(k, 2) * 2 + c
        for half in range(PIECES // 2):
            arrived(r_piece(far, 2 * half), y2_recv.at[0, k, half])
            arrived(r_piece(far, 2 * half + 1), y2_recv.at[1, k, half])
        hand_over(k, 2)

    for half in range(PIECES // 2):
        y_second(1, half)
        flip, dy = ((0, 0), (0, up), (0, down), (1, 0))[half]
        if half:
            ready_rows(flip, dy)
        each(2, lambda slot: tile(r_pair(flip, dy), slot))
    hand_over(1, up)
    hand_over(1, down)
    for half in range(PIECES // 2):
        z_second(1, half)
        if half == 0:
            y_last(0)
        else:
            flip, dy = ((1, up), (1, down), (0, 2))[half - 1]
            ready_rows(flip, dy)
            each(2, lambda slot: tile(r_pair(flip, dy), slot))
    ready_columns(2)
    y_last(1)
    each(7, lambda t: tile(r_pair(t % 2, turn(t // 2)), 2))
    ready_rows(1, 2)
    each(3, lambda slot: tile(r_pair(1, 2), slot))

    q = c_pair(2)
    columns = pl.ds(pl.multiple_of(q * PAIR, PAIR), PAIR)
    for half in range(PIECES // 2):
        for k in range(2):
            arrived(c_piece(q * 2 + k, 2 * half), z2_recv.at[0, (k + b + 1) % 2, half])
            arrived(c_piece(q * 2 + k, 2 * half + 1), z2_recv.at[1, (k + b + 1) % 2, half])
        deep = slice(2 * half * DEEP, 2 * (half + 1) * DEEP)
        for k in range(2):
            to = slice(k * BLOCK, (k + 1) * BLOCK)
            v = cbuf[q * 2 + k, deep, :]
            hi = v.astype(jnp.bfloat16)
            chi[3, deep, to] = hi
            clo[3, deep, to] = (v - hi.astype(jnp.float32)).astype(jnp.bfloat16)

        def part(m):
            rows = pl.ds(pl.multiple_of(m * 2 * PAIR, 2 * PAIR), 2 * PAIR)
            left, right = rhi[rows, deep], chi[3, deep, :]
            total = dot(left, right) + dot(left, clo[3, deep, :]) + dot(rlo[rows, deep], right)
            total = total * (1.0 / SAMPLES)
            outbuf[rows, columns] = total if half == 0 else outbuf[rows, columns] + total
            if half == PIECES // 2 - 1:
                pltpu.make_async_copy(outbuf.at[rows, columns], out_ref.at[rows, columns], out_sem).start()

        each(4, part)

    for sem, blocks in ((S_T, 1), (S_X, 1), (S_B, 1), (S_YU, 3), (S_YD, 3), (S_ZU, 3), (S_ZD, 3), (S_D, 8)):
        arrived(rbuf.at[pl.ds(0, blocks)], send.at[sem])

    @pl.when(off == 0)
    def _():
        arrived(rbuf.at[0], send.at[S_TR])

    @pl.when(off == 2)
    def _():
        arrived(rbuf.at[0, pl.ds(0, BLOCK // 2), :], send.at[S_TR])

    pltpu.make_async_copy(outbuf, out_ref, out_sem).wait()


def local(loadings):
    dma = pltpu.SemaphoreType.DMA
    return pl.pallas_call(
        kernel,
        out_shape=jax.ShapeDtypeStruct((16 * BLOCK, 8 * BLOCK), jnp.float32),
        in_specs=[pl.BlockSpec(memory_space=pltpu.VMEM)],
        out_specs=pl.BlockSpec(memory_space=pl.ANY),
        scratch_shapes=[
            pltpu.VMEM((16, BLOCK, DEPTH), jnp.float32),
            pltpu.VMEM((8, DEPTH, BLOCK), jnp.float32),
            pltpu.VMEM((DEPTH, BLOCK), jnp.float32),
            pltpu.VMEM((2, PIECES // 2, DEEP, BLOCK), jnp.float32),
            pltpu.VMEM((8 * PAIR, DEPTH), jnp.bfloat16),
            pltpu.VMEM((8 * PAIR, DEPTH), jnp.bfloat16),
            pltpu.VMEM((4, DEPTH, PAIR), jnp.bfloat16),
            pltpu.VMEM((4, DEPTH, PAIR), jnp.bfloat16),
            pltpu.VMEM((16 * BLOCK, 8 * BLOCK), jnp.float32),
            dma((9,)),
            dma((PIECES,)),
            dma((2, PIECES // 2)),
            dma((PIECES,)),
            dma((PIECES,)),
            dma((2, 2, PIECES)),
            dma((2, 2, PIECES // 2)),
            dma((2, 2, PIECES)),
            dma((2, 2, PIECES // 2)),
            dma((8,)),
            dma,
        ],
        compiler_params=pltpu.CompilerParams(
            collective_id=0, has_side_effects=True, vmem_limit_bytes=61 * 1024 * 1024
        ),
    )(loadings)


def solution(mesh):
    placed = (P(None, None, ("row", "col")),)
    return jax.shard_map(local, mesh=mesh, in_specs=placed, out_specs=P("row", "col"), check_vma=False)
```

```python
import functools

import jax
import jax.numpy as jnp
from jax import lax
from jax.experimental import pallas as pl
from jax.experimental.pallas import tpu as pltpu
from jax.sharding import PartitionSpec as P

MESH = pl.DeviceIdType.MESH
SAMPLES, FACTORS, BLOCK = 64, 32, 128
DEPTH = SAMPLES * FACTORS
PIECES = 8
ROWS = BLOCK // PIECES
DEEP = DEPTH // PIECES
PAIR = 2 * BLOCK


def place(a, b, y, z, c):
    return (b * 4 + z, a * 8 + y * 2 + c)


def kernel(
    x_ref,
    outbuf,
    rbuf,
    cbuf,
    csend,
    tbuf,
    rhi,
    rlo,
    chi,
    clo,
    send,
    t_recv,
    tr_recv,
    x_recv,
    b_recv,
    y1_recv,
    y2_recv,
    z1_recv,
    z2_recv,
    d_recv,
):
    row, col = lax.axis_index("row"), lax.axis_index("col")
    b, z = row // 4, row % 4
    a, y, c = col // 8, (col // 2) % 4, col % 2
    up, down = 1, 3

    twin = place(a, b, y, z, 1 - c)
    across = place(1 - a, b, y, z, c)
    beside = place(a, 1 - b, y, z, c)
    y_dev = {d: place(a, b, (y + d) % 4, z, c) for d in (up, down)}
    z_dev = {d: place(a, b, y, (z + d) % 4, c) for d in (up, down)}
    t_to = place(b, 1 - c, z, (2 * z + 4 - y) % 4, a)
    t_from = place(c, a, (2 * y + 4 - z) % 4, y, 1 - b)
    off = (y + 4 - z) % 4
    turns = (1, 3)

    def corner_from(e):
        return place(c, a, (y + 6 - e) % 4, (z + 4 - e) % 4, 1 - b)

    def corner_to(e):
        return place(a, b, (y + 4 - e) % 4, (z + 6 - e) % 4, c)

    def side_from(d):
        return place(c, a, y, (y + 4 - d) % 4, 1 - b)

    def side_to(d):
        return place(a, b, (y + 4 - d) % 4, z, c)

    def r_pair(flip, dy):
        return (a + flip) % 2 * 4 + (y + dy) % 4

    def c_pair(dz):
        return (2 * y + 8 - z - dz) % 4

    barrier = pltpu.get_barrier_semaphore()

    def here(*devices):
        for device in devices:
            pl.semaphore_signal(barrier, inc=1, device_id=device, device_id_type=MESH)

    here(twin, across, beside, y_dev[up], y_dev[down], z_dev[up], z_dev[down], t_from)

    @pl.when(off % 2 == 1)
    def _():
        here(place(a, b, (y + off) % 4, z, c))

    @pl.when(off == 2)
    def _():
        here(*(side_from(d) for d in turns))
        here(*(place(a, b, (y + e) % 4, (y + e) % 4, c) for e in turns))

    @pl.when(off == 0)
    def _():
        here(*(corner_from(e) for e in turns))

    own = r_pair(0, 0) * 2 + c

    def normalise(i, _):
        x = x_ref[pl.ds(i * 8, 8)]
        variance = jnp.sum(x * x, axis=1, keepdims=True)
        scaled = (x * (1.0 / jnp.sqrt(variance))).reshape(8 * FACTORS, BLOCK)
        at = pl.ds(pl.multiple_of(i * 8 * FACTORS, 8 * FACTORS), 8 * FACTORS)
        csend[at, :] = scaled
        rbuf[own, :, at] = scaled.T
        return 0

    lax.fori_loop(0, SAMPLES // 8, normalise, 0)
    odd = off % 2
    pl.semaphore_wait(barrier, 8 + odd + (1 - odd) * (2 + 2 * (off // 2)))

    def go(src, dst, sem, recv, device):
        pltpu.make_async_remote_copy(
            src_ref=src, dst_ref=dst, send_sem=send.at[sem], recv_sem=recv, device_id=device, device_id_type=MESH
        ).start()

    def r_piece(block, i):
        return rbuf.at[block, pl.ds(i * ROWS, ROWS), :]

    def c_piece(block, i):
        return cbuf.at[block, pl.ds(i * DEEP, DEEP), :]

    def arrived(ref, sem):
        pltpu.make_async_copy(ref, ref, sem).wait()

    def r_go(block, i, sem, recv, device):
        go(r_piece(block, i), r_piece(block, i), sem, recv, device)

    def c_go(block, i, sem, recv, device):
        go(c_piece(block, i), c_piece(block, i), sem, recv, device)

    S_T, S_X, S_B, S_YU, S_YD, S_ZU, S_ZD, S_D, S_TR = range(9)

    def hand_over(flip, dy):
        pair = r_pair(flip, dy)
        go(rbuf.at[pair * 2 + c], rbuf.at[pair * 2 + c], S_D, d_recv.at[pair], twin)

    def y_first(k, i):
        block = r_pair(k, 0) * 2 + c
        r_go(block, i, S_YU, y1_recv.at[0, k, i], y_dev[up])
        r_go(block, i, S_YD, y1_recv.at[1, k, i], y_dev[down])

    def z_first(k, block, i):
        c_go(block, i, S_ZU, z1_recv.at[0, k, i], z_dev[up])
        c_go(block, i, S_ZD, z1_recv.at[1, k, i], z_dev[down])

    def each(n, body):
        def step(i, _):
            body(i)
            return 0

        lax.fori_loop(0, n, step, 0)

    t_slot = y * 2 + c
    own_t = c_pair(0) * 2 + 1 - b
    own_b = c_pair(0) * 2 + b

    def transposed(i):
        src = csend.at[pl.ds(i * DEEP, DEEP), :]
        aside = (off % 2) * (i % 4 // 3) + (off // 2) * (1 - off % 2)
        f, slot = i % 2, i // 2

        @pl.when(aside == 0)
        def _():
            go(src, c_piece(t_slot, i), S_T, t_recv.at[i], t_to)

        @pl.when(aside * (off % 2) == 1)
        def _():
            g = off // 2
            go(src, tbuf.at[g, i // 4], S_T, tr_recv.at[g, i // 4], place(b, 1 - c, y, (z + 4 - off) % 4, a))

        @pl.when(aside * (1 - off % 2) == 1)
        def _():
            w = (z + 1 + 2 * f) % 4
            go(src, tbuf.at[f, slot], S_T, tr_recv.at[f, slot], place(b, 1 - c, w, w, a))

    def start(i):
        @pl.when(i < 3)
        def _():
            y_first(0, i)

    def pass_corner(i):
        f, slot = i % 2, i // 2

        @pl.when(off == 0)
        def _():
            e = 1 + 2 * f
            arrived(tbuf.at[f, slot], tr_recv.at[f, slot])
            at = (y + 6 - e) % 4 * 2 + 1 - b
            go(tbuf.at[f, slot], c_piece(at, i), S_TR, t_recv.at[i], corner_to(e))

    def pass_side(i):
        f, slot = i % 2, i // 2

        @pl.when((off // 2) * (1 - off % 2) * (1 - i // 4) == 1)
        def _():
            arrived(tbuf.at[f, slot], tr_recv.at[f, slot])
            p = 4 * slot + 3
            go(tbuf.at[f, slot], c_piece(y * 2 + 1 - b, p), S_TR, t_recv.at[p], side_to(1 + 2 * f))

    each(PIECES, transposed)
    each(PIECES, start)
    hand_over(0, 0)

    def split_rows(pair, half):
        def body(i):
            at = pl.ds(pl.multiple_of(i * 16, 16), 16)
            v = rbuf[pair * 2 + half, at, :]
            hi = v.astype(jnp.bfloat16)
            to = pl.ds(pl.multiple_of(pair * PAIR + half * BLOCK + i * 16, 16), 16)
            rhi[to, :] = hi
            rlo[to, :] = (v - hi.astype(jnp.float32)).astype(jnp.bfloat16)

        each(BLOCK // 16, body)

    def ready_rows(flip, dy):
        pair = r_pair(flip, dy)
        arrived(rbuf.at[pair * 2 + 1 - c], d_recv.at[pair])
        split_rows(pair, 0)
        split_rows(pair, 1)

    def blocks_of(slot):
        beyond = (slot + 1) // 2
        which = (slot + b) % 2
        left = (1 - beyond) * (c_pair(0) * 2) + beyond * (c_pair(up) * 2 + which)
        right = (1 - beyond) * (c_pair(0) * 2 + 1) + beyond * (c_pair(down) * 2 + which)
        return left, right

    def ready_columns(slot):
        for side, block in enumerate(blocks_of(slot)):

            def body(i):
                at = pl.ds(pl.multiple_of(i * DEEP, DEEP), DEEP)
                v = cbuf[block, at, :]
                hi = v.astype(jnp.bfloat16)
                to = slice(side * BLOCK, (side + 1) * BLOCK)
                chi[slot, at, to] = hi
                clo[slot, at, to] = (v - hi.astype(jnp.float32)).astype(jnp.bfloat16)

            each(PIECES, body)

    def dot(left, right):
        return jnp.dot(left, right, preferred_element_type=jnp.float32)

    def tile(p, slot):
        rows = pl.ds(pl.multiple_of(p * PAIR, PAIR), PAIR)
        right = chi[slot]
        total = dot(rhi[rows, :], right) + dot(rhi[rows, :], clo[slot]) + dot(rlo[rows, :], right)
        total = total * (1.0 / SAMPLES)
        for side, block in enumerate(blocks_of(slot)):
            columns = pl.ds(pl.multiple_of(block * BLOCK, BLOCK), BLOCK)
            outbuf[rows, columns] = total[:, side * BLOCK : (side + 1) * BLOCK]

    def turn(m):
        return m + m // 2 - 2 * (m // 3)

    ready_rows(0, 0)

    def y_second(k, half):
        even, odd = 2 * half, 2 * half + 1
        below, above = r_pair(k, down) * 2 + c, r_pair(k, up) * 2 + c
        for i in (even, odd):
            arrived(r_piece(below, i), y1_recv.at[0, k, i])
            arrived(r_piece(above, i), y1_recv.at[1, k, i])
        r_go(below, even, S_YU, y2_recv.at[0, k, half], y_dev[up])
        r_go(above, odd, S_YD, y2_recv.at[1, k, half], y_dev[down])

    def z_second(k, half):
        even, odd = 2 * half, 2 * half + 1
        s = (1 - b + k) % 2
        below, above = c_pair(down) * 2 + s, c_pair(up) * 2 + s
        for i in (even, odd):
            arrived(c_piece(below, i), z1_recv.at[0, k, i])
            arrived(c_piece(above, i), z1_recv.at[1, k, i])
        c_go(below, even, S_ZU, z2_recv.at[0, k, half], z_dev[up])
        c_go(above, odd, S_ZD, z2_recv.at[1, k, half], z_dev[down])

    def early(i):
        @pl.when((off // 2) * (1 - off % 2) * (i % 2) == 1)
        def _():
            z_second(0, i // 2)

        pass_side(i)
        arrived(c_piece(own_t, i), t_recv.at[i])
        z_first(0, own_t, i)
        c_go(own_t, i, S_B, b_recv.at[i], beside)
        r_go(own, i, S_X, x_recv.at[i], across)
        pass_corner(i)

        @pl.when(i < PIECES - 3)
        def _():
            y_first(0, i + 3)

        @pl.when(i >= PIECES // 2)
        def _():
            y_second(0, i - PIECES // 2)

            @pl.when(off == 0)
            def _():
                z_second(0, i - PIECES // 2)

    each(PIECES, early)

    def middle(i):
        arrived(r_piece(r_pair(1, 0) * 2 + c, i), x_recv.at[i])
        y_first(1, i)

        @pl.when((i % 2) * (off % 2) == 1)
        def _():
            z_second(0, i // 2)

        arrived(c_piece(own_b, i), b_recv.at[i])
        z_first(1, own_b, i)

    each(PIECES, middle)
    hand_over(0, up)
    hand_over(0, down)
    hand_over(1, 0)
    ready_columns(0)
    ready_columns(1)

    def y_last(k):
        far = r_pair(k, 2) * 2 + c
        for half in range(PIECES // 2):
            arrived(r_piece(far, 2 * half), y2_recv.at[0, k, half])
            arrived(r_piece(far, 2 * half + 1), y2_recv.at[1, k, half])
        hand_over(k, 2)

    for half in range(PIECES // 2):
        y_second(1, half)
        flip, dy = ((0, 0), (0, up), (0, down), (1, 0))[half]
        if half:
            ready_rows(flip, dy)
        each(2, lambda slot: tile(r_pair(flip, dy), slot))
    hand_over(1, up)
    hand_over(1, down)
    for half in range(PIECES // 2):
        z_second(1, half)
        if half == 0:
            y_last(0)
        else:
            flip, dy = ((1, up), (1, down), (0, 2))[half - 1]
            ready_rows(flip, dy)
            each(2, lambda slot: tile(r_pair(flip, dy), slot))
    ready_columns(2)
    y_last(1)
    each(7, lambda t: tile(r_pair(t % 2, turn(t // 2)), 2))
    ready_rows(1, 2)
    each(3, lambda slot: tile(r_pair(1, 2), slot))

    q = c_pair(2)
    columns = pl.ds(pl.multiple_of(q * PAIR, PAIR), PAIR)
    for half in range(PIECES // 2):
        for k in range(2):
            arrived(c_piece(q * 2 + k, 2 * half), z2_recv.at[0, (k + b + 1) % 2, half])
            arrived(c_piece(q * 2 + k, 2 * half + 1), z2_recv.at[1, (k + b + 1) % 2, half])
        deep = slice(2 * half * DEEP, 2 * (half + 1) * DEEP)
        for k in range(2):
            to = slice(k * BLOCK, (k + 1) * BLOCK)
            v = cbuf[q * 2 + k, deep, :]
            hi = v.astype(jnp.bfloat16)
            chi[3, deep, to] = hi
            clo[3, deep, to] = (v - hi.astype(jnp.float32)).astype(jnp.bfloat16)

        def part(m):
            rows = pl.ds(pl.multiple_of(m * 2 * PAIR, 2 * PAIR), 2 * PAIR)
            left, right = rhi[rows, deep], chi[3, deep, :]
            total = dot(left, right) + dot(left, clo[3, deep, :]) + dot(rlo[rows, deep], right)
            total = total * (1.0 / SAMPLES)
            outbuf[rows, columns] = total if half == 0 else outbuf[rows, columns] + total

        each(4, part)

    for sem, blocks in ((S_T, 1), (S_X, 1), (S_B, 1), (S_YU, 3), (S_YD, 3), (S_ZU, 3), (S_ZD, 3), (S_D, 8)):
        arrived(rbuf.at[pl.ds(0, blocks)], send.at[sem])

    @pl.when(off == 0)
    def _():
        arrived(rbuf.at[0], send.at[S_TR])

    @pl.when(off == 2)
    def _():
        arrived(rbuf.at[0, pl.ds(0, BLOCK // 2), :], send.at[S_TR])


def write_out(held, out_ref, sem):
    for i in range(8):
        rows = pl.ds(i * PAIR, PAIR)
        pltpu.make_async_copy(held.at[rows], out_ref.at[rows], sem).start()
    pltpu.make_async_copy(held, out_ref, sem).wait()


def local(loadings):
    dma = pltpu.SemaphoreType.DMA
    held = pl.pallas_call(
        kernel,
        out_shape=pltpu.VMEM((16 * BLOCK, 8 * BLOCK), jnp.float32),
        in_specs=[pl.BlockSpec(memory_space=pltpu.VMEM)],
        out_specs=pl.BlockSpec(memory_space=pltpu.VMEM),
        scratch_shapes=[
            pltpu.VMEM((16, BLOCK, DEPTH), jnp.float32),
            pltpu.VMEM((8, DEPTH, BLOCK), jnp.float32),
            pltpu.VMEM((DEPTH, BLOCK), jnp.float32),
            pltpu.VMEM((2, PIECES // 2, DEEP, BLOCK), jnp.float32),
            pltpu.VMEM((8 * PAIR, DEPTH), jnp.bfloat16),
            pltpu.VMEM((8 * PAIR, DEPTH), jnp.bfloat16),
            pltpu.VMEM((4, DEPTH, PAIR), jnp.bfloat16),
            pltpu.VMEM((4, DEPTH, PAIR), jnp.bfloat16),
            dma((9,)),
            dma((PIECES,)),
            dma((2, PIECES // 2)),
            dma((PIECES,)),
            dma((PIECES,)),
            dma((2, 2, PIECES)),
            dma((2, 2, PIECES // 2)),
            dma((2, 2, PIECES)),
            dma((2, 2, PIECES // 2)),
            dma((8,)),
        ],
        compiler_params=pltpu.CompilerParams(
            collective_id=0, has_side_effects=True, vmem_limit_bytes=54 * 1024 * 1024
        ),
    )(loadings)
    return pl.pallas_call(
        write_out,
        out_shape=jax.ShapeDtypeStruct(held.shape, held.dtype),
        in_specs=[pl.BlockSpec(memory_space=pltpu.VMEM)],
        out_specs=pl.BlockSpec(memory_space=pl.ANY),
        scratch_shapes=[dma],
        compiler_params=pltpu.CompilerParams(vmem_limit_bytes=1024 * 1024),
    )(held)


def solution(mesh):
    placed = (P(None, None, ("row", "col")),)
    return jax.shard_map(local, mesh=mesh, in_specs=placed, out_specs=P("row", "col"), check_vma=False)
```

```python
import functools

import jax
import jax.numpy as jnp
from jax import lax
from jax.experimental import pallas as pl
from jax.experimental.pallas import tpu as pltpu
from jax.sharding import PartitionSpec as P

MESH = pl.DeviceIdType.MESH
SAMPLES, FACTORS, BLOCK = 64, 32, 128
DEPTH = SAMPLES * FACTORS
PIECES = 8
ROWS = BLOCK // PIECES
DEEP = DEPTH // PIECES
PAIR = 2 * BLOCK


def place(a, b, y, z, c):
    return (b * 4 + z, a * 8 + y * 2 + c)


def kernel(
    x_ref,
    outbuf,
    rbuf,
    cbuf,
    csend,
    tbuf,
    rhi,
    rlo,
    chi,
    clo,
    send,
    t_recv,
    tr_recv,
    x_recv,
    b_recv,
    y1_recv,
    y2_recv,
    z1_recv,
    z2_recv,
    d_recv,
):
    row, col = lax.axis_index("row"), lax.axis_index("col")
    b, z = row // 4, row % 4
    a, y, c = col // 8, (col // 2) % 4, col % 2
    up, down = 1, 3

    twin = place(a, b, y, z, 1 - c)
    across = place(1 - a, b, y, z, c)
    beside = place(a, 1 - b, y, z, c)
    y_dev = {d: place(a, b, (y + d) % 4, z, c) for d in (up, down)}
    z_dev = {d: place(a, b, y, (z + d) % 4, c) for d in (up, down)}
    t_to = place(b, 1 - c, z, (2 * z + 4 - y) % 4, a)
    t_from = place(c, a, (2 * y + 4 - z) % 4, y, 1 - b)
    off = (y + 4 - z) % 4
    turns = (1, 3)

    def corner_from(e):
        return place(c, a, (y + 6 - e) % 4, (z + 4 - e) % 4, 1 - b)

    def corner_to(e):
        return place(a, b, (y + 4 - e) % 4, (z + 6 - e) % 4, c)

    def side_from(d):
        return place(c, a, y, (y + 4 - d) % 4, 1 - b)

    def side_to(d):
        return place(a, b, (y + 4 - d) % 4, z, c)

    def r_pair(flip, dy):
        return (a + flip) % 2 * 4 + (y + dy) % 4

    def c_pair(dz):
        return (2 * y + 8 - z - dz) % 4

    barrier = pltpu.get_barrier_semaphore()

    def here(*devices):
        for device in devices:
            pl.semaphore_signal(barrier, inc=1, device_id=device, device_id_type=MESH)

    here(twin, across, beside, y_dev[up], y_dev[down], z_dev[up], z_dev[down], t_from)

    @pl.when(off % 2 == 1)
    def _():
        here(place(a, b, (y + off) % 4, z, c))

    @pl.when(off == 2)
    def _():
        here(*(side_from(d) for d in turns))
        here(*(place(a, b, (y + e) % 4, (y + e) % 4, c) for e in turns))

    @pl.when(off == 0)
    def _():
        here(*(corner_from(e) for e in turns))

    own = r_pair(0, 0) * 2 + c

    def normalise(i, _):
        x = x_ref[pl.ds(i * 8, 8)]
        variance = jnp.sum(x * x, axis=1, keepdims=True)
        scaled = (x * (1.0 / jnp.sqrt(variance))).reshape(8 * FACTORS, BLOCK)
        at = pl.ds(pl.multiple_of(i * 8 * FACTORS, 8 * FACTORS), 8 * FACTORS)
        csend[at, :] = scaled
        rbuf[own, :, at] = scaled.T
        return 0

    lax.fori_loop(0, SAMPLES // 8, normalise, 0)
    odd = off % 2
    pl.semaphore_wait(barrier, 8 + odd + (1 - odd) * (2 + 2 * (off // 2)))

    def go(src, dst, sem, recv, device):
        pltpu.make_async_remote_copy(
            src_ref=src, dst_ref=dst, send_sem=send.at[sem], recv_sem=recv, device_id=device, device_id_type=MESH
        ).start()

    def r_piece(block, i):
        return rbuf.at[block, pl.ds(i * ROWS, ROWS), :]

    def c_piece(block, i):
        return cbuf.at[block, pl.ds(i * DEEP, DEEP), :]

    def arrived(ref, sem):
        pltpu.make_async_copy(ref, ref, sem).wait()

    def r_go(block, i, sem, recv, device):
        go(r_piece(block, i), r_piece(block, i), sem, recv, device)

    def c_go(block, i, sem, recv, device):
        go(c_piece(block, i), c_piece(block, i), sem, recv, device)

    S_T, S_X, S_B, S_YU, S_YD, S_ZU, S_ZD, S_D, S_TR = range(9)

    def hand_over(flip, dy):
        pair = r_pair(flip, dy)
        go(rbuf.at[pair * 2 + c], rbuf.at[pair * 2 + c], S_D, d_recv.at[pair], twin)

    def y_first(k, i):
        block = r_pair(k, 0) * 2 + c
        r_go(block, i, S_YU, y1_recv.at[0, k, i], y_dev[up])
        r_go(block, i, S_YD, y1_recv.at[1, k, i], y_dev[down])

    def z_first(k, block, i):
        c_go(block, i, S_ZU, z1_recv.at[0, k, i], z_dev[up])
        c_go(block, i, S_ZD, z1_recv.at[1, k, i], z_dev[down])

    def each(n, body):
        def step(i, _):
            body(i)
            return 0

        lax.fori_loop(0, n, step, 0)

    t_slot = y * 2 + c
    own_t = c_pair(0) * 2 + 1 - b
    own_b = c_pair(0) * 2 + b

    def transposed(i):
        src = csend.at[pl.ds(i * DEEP, DEEP), :]
        aside = (off % 2) * (i % 4 // 3) + (off // 2) * (1 - off % 2)
        f, slot = i % 2, i // 2

        @pl.when(aside == 0)
        def _():
            go(src, c_piece(t_slot, i), S_T, t_recv.at[i], t_to)

        @pl.when(aside * (off % 2) == 1)
        def _():
            g = off // 2
            go(src, tbuf.at[g, i // 4], S_T, tr_recv.at[g, i // 4], place(b, 1 - c, y, (z + 4 - off) % 4, a))

        @pl.when(aside * (1 - off % 2) == 1)
        def _():
            w = (z + 1 + 2 * f) % 4
            go(src, tbuf.at[f, slot], S_T, tr_recv.at[f, slot], place(b, 1 - c, w, w, a))

    def start(i):
        @pl.when(i < 3)
        def _():
            y_first(0, i)

    def pass_corner(i):
        f, slot = i % 2, i // 2

        @pl.when(off == 0)
        def _():
            e = 1 + 2 * f
            arrived(tbuf.at[f, slot], tr_recv.at[f, slot])
            at = (y + 6 - e) % 4 * 2 + 1 - b
            go(tbuf.at[f, slot], c_piece(at, i), S_TR, t_recv.at[i], corner_to(e))

    def pass_side(i):
        f, slot = i % 2, i // 2

        @pl.when((off // 2) * (1 - off % 2) * (1 - i // 4) == 1)
        def _():
            arrived(tbuf.at[f, slot], tr_recv.at[f, slot])
            p = 4 * slot + 3
            go(tbuf.at[f, slot], c_piece(y * 2 + 1 - b, p), S_TR, t_recv.at[p], side_to(1 + 2 * f))

    each(PIECES, transposed)
    each(PIECES, start)
    hand_over(0, 0)

    def split_rows(pair, half):
        def body(i):
            at = pl.ds(pl.multiple_of(i * 16, 16), 16)
            v = rbuf[pair * 2 + half, at, :]
            hi = v.astype(jnp.bfloat16)
            to = pl.ds(pl.multiple_of(pair * PAIR + half * BLOCK + i * 16, 16), 16)
            rhi[to, :] = hi
            rlo[to, :] = (v - hi.astype(jnp.float32)).astype(jnp.bfloat16)

        each(BLOCK // 16, body)

    def ready_rows(flip, dy):
        pair = r_pair(flip, dy)
        arrived(rbuf.at[pair * 2 + 1 - c], d_recv.at[pair])
        split_rows(pair, 0)
        split_rows(pair, 1)

    def blocks_of(slot):
        beyond = (slot + 1) // 2
        which = (slot + b) % 2
        left = (1 - beyond) * (c_pair(0) * 2) + beyond * (c_pair(up) * 2 + which)
        right = (1 - beyond) * (c_pair(0) * 2 + 1) + beyond * (c_pair(down) * 2 + which)
        return left, right

    def split_columns(species, slot, side, i):
        at = pl.ds(pl.multiple_of(i * DEEP, DEEP), DEEP)
        v = cbuf[species, at, :]
        hi = v.astype(jnp.bfloat16)
        to = slice(side * BLOCK, (side + 1) * BLOCK)
        chi[slot, at, to] = hi
        clo[slot, at, to] = (v - hi.astype(jnp.float32)).astype(jnp.bfloat16)

    def ready_columns(slot):
        for side, species in enumerate(blocks_of(slot)):
            each(PIECES, lambda i: split_columns(species, slot, side, i))

    def dot(left, right):
        return jnp.dot(left, right, preferred_element_type=jnp.float32)

    def block(start, n, slot, columns_of):
        rows = pl.ds(pl.multiple_of(start * PAIR, PAIR), n * PAIR)
        right = chi[slot]
        total = dot(rhi[rows, :], right) + dot(rhi[rows, :], clo[slot]) + dot(rlo[rows, :], right)
        total = total * (1.0 / SAMPLES)
        for side, species in enumerate(columns_of):
            columns = pl.ds(pl.multiple_of(species * BLOCK, BLOCK), BLOCK)
            outbuf[rows, columns] = total[:, side * BLOCK : (side + 1) * BLOCK]

    def tile(p, slot):
        block(p, 1, slot, blocks_of(slot))

    def turn(m):
        return m + m // 2 - 2 * (m // 3)

    ready_rows(0, 0)

    def y_second(k, half):
        even, odd = 2 * half, 2 * half + 1
        below, above = r_pair(k, down) * 2 + c, r_pair(k, up) * 2 + c
        for i in (even, odd):
            arrived(r_piece(below, i), y1_recv.at[0, k, i])
            arrived(r_piece(above, i), y1_recv.at[1, k, i])
        r_go(below, even, S_YU, y2_recv.at[0, k, half], y_dev[up])
        r_go(above, odd, S_YD, y2_recv.at[1, k, half], y_dev[down])

    def z_second(k, half):
        even, odd = 2 * half, 2 * half + 1
        s = (1 - b + k) % 2
        below, above = c_pair(down) * 2 + s, c_pair(up) * 2 + s
        for i in (even, odd):
            arrived(c_piece(below, i), z1_recv.at[0, k, i])
            arrived(c_piece(above, i), z1_recv.at[1, k, i])
        c_go(below, even, S_ZU, z2_recv.at[0, k, half], z_dev[up])
        c_go(above, odd, S_ZD, z2_recv.at[1, k, half], z_dev[down])

    def early(i):
        @pl.when((off // 2) * (1 - off % 2) * (i % 2) == 1)
        def _():
            z_second(0, i // 2)

        pass_side(i)
        arrived(c_piece(own_t, i), t_recv.at[i])
        z_first(0, own_t, i)
        c_go(own_t, i, S_B, b_recv.at[i], beside)
        r_go(own, i, S_X, x_recv.at[i], across)
        pass_corner(i)

        @pl.when(i < PIECES - 3)
        def _():
            y_first(0, i + 3)

        @pl.when(i >= PIECES // 2)
        def _():
            y_second(0, i - PIECES // 2)

            @pl.when(off == 0)
            def _():
                z_second(0, i - PIECES // 2)

    each(PIECES, early)

    def middle(i):
        arrived(r_piece(r_pair(1, 0) * 2 + c, i), x_recv.at[i])
        y_first(1, i)

        @pl.when((i % 2) * (off % 2) == 1)
        def _():
            z_second(0, i // 2)

        arrived(c_piece(own_b, i), b_recv.at[i])
        z_first(1, own_b, i)

    each(PIECES, middle)
    hand_over(0, up)
    hand_over(0, down)
    hand_over(1, 0)
    ready_columns(0)
    ready_columns(1)

    def y_last(k):
        far = r_pair(k, 2) * 2 + c
        for half in range(PIECES // 2):
            arrived(r_piece(far, 2 * half), y2_recv.at[0, k, half])
            arrived(r_piece(far, 2 * half + 1), y2_recv.at[1, k, half])
        hand_over(k, 2)

    for half in range(PIECES // 2):
        y_second(1, half)
        flip, dy = ((0, 0), (0, up), (0, down), (1, 0))[half]
        if half:
            ready_rows(flip, dy)
        each(2, lambda slot: tile(r_pair(flip, dy), slot))
    hand_over(1, up)
    hand_over(1, down)
    for half in range(PIECES // 2):
        z_second(1, half)
        if half == 0:
            y_last(0)
        else:
            flip, dy = ((1, up), (1, down), (0, 2))[half - 1]
            ready_rows(flip, dy)
            each(2, lambda slot: tile(r_pair(flip, dy), slot))
    y_last(1)
    ready_columns(2)
    last = r_pair(1, 2)
    each(3, lambda m: block((last // 2 + 1 + m) % 4 * 2, 2, 2, blocks_of(2)))
    ready_rows(1, 2)
    block(last // 2 * 2, 2, 2, blocks_of(2))
    each(2, lambda slot: tile(last, slot))

    far = (c_pair(2) * 2, c_pair(2) * 2 + 1)
    for k in range(2):
        species = c_pair(2) * 2 + (1 - b + k) % 2
        for half in range(PIECES // 2):
            arrived(c_piece(species, 2 * half), z2_recv.at[0, k, half])
            arrived(c_piece(species, 2 * half + 1), z2_recv.at[1, k, half])
    for side in range(2):
        each(PIECES, lambda i: split_columns(far[side], 0, side, i))
    each(4, lambda m: block(m * 2, 2, 0, far))

    for sem, blocks in ((S_T, 1), (S_X, 1), (S_B, 1), (S_YU, 3), (S_YD, 3), (S_ZU, 3), (S_ZD, 3), (S_D, 8)):
        arrived(rbuf.at[pl.ds(0, blocks)], send.at[sem])

    @pl.when(off == 0)
    def _():
        arrived(rbuf.at[0], send.at[S_TR])

    @pl.when(off == 2)
    def _():
        arrived(rbuf.at[0, pl.ds(0, BLOCK // 2), :], send.at[S_TR])


def write_out(held, out_ref, sem):
    for i in range(8):
        rows = pl.ds(i * PAIR, PAIR)
        pltpu.make_async_copy(held.at[rows], out_ref.at[rows], sem).start()
    pltpu.make_async_copy(held, out_ref, sem).wait()


def local(loadings):
    dma = pltpu.SemaphoreType.DMA
    held = pl.pallas_call(
        kernel,
        out_shape=pltpu.VMEM((16 * BLOCK, 8 * BLOCK), jnp.float32),
        in_specs=[pl.BlockSpec(memory_space=pltpu.VMEM)],
        out_specs=pl.BlockSpec(memory_space=pltpu.VMEM),
        scratch_shapes=[
            pltpu.VMEM((16, BLOCK, DEPTH), jnp.float32),
            pltpu.VMEM((8, DEPTH, BLOCK), jnp.float32),
            pltpu.VMEM((DEPTH, BLOCK), jnp.float32),
            pltpu.VMEM((2, PIECES // 2, DEEP, BLOCK), jnp.float32),
            pltpu.VMEM((8 * PAIR, DEPTH), jnp.bfloat16),
            pltpu.VMEM((8 * PAIR, DEPTH), jnp.bfloat16),
            pltpu.VMEM((3, DEPTH, PAIR), jnp.bfloat16),
            pltpu.VMEM((3, DEPTH, PAIR), jnp.bfloat16),
            dma((9,)),
            dma((PIECES,)),
            dma((2, PIECES // 2)),
            dma((PIECES,)),
            dma((PIECES,)),
            dma((2, 2, PIECES)),
            dma((2, 2, PIECES // 2)),
            dma((2, 2, PIECES)),
            dma((2, 2, PIECES // 2)),
            dma((8,)),
        ],
        compiler_params=pltpu.CompilerParams(
            collective_id=0, has_side_effects=True, vmem_limit_bytes=54 * 1024 * 1024
        ),
    )(loadings)
    return pl.pallas_call(
        write_out,
        out_shape=jax.ShapeDtypeStruct(held.shape, held.dtype),
        in_specs=[pl.BlockSpec(memory_space=pltpu.VMEM)],
        out_specs=pl.BlockSpec(memory_space=pl.ANY),
        scratch_shapes=[dma],
        compiler_params=pltpu.CompilerParams(vmem_limit_bytes=1024 * 1024),
    )(held)


def solution(mesh):
    placed = (P(None, None, ("row", "col")),)
    return jax.shard_map(local, mesh=mesh, in_specs=placed, out_specs=P("row", "col"), check_vma=False)
```

```python
import functools

import jax
import jax.numpy as jnp
from jax import lax
from jax.experimental import pallas as pl
from jax.experimental.pallas import tpu as pltpu
from jax.sharding import PartitionSpec as P

MESH = pl.DeviceIdType.MESH
SAMPLES, FACTORS, BLOCK = 64, 32, 128
DEPTH = SAMPLES * FACTORS
PIECES = 8
ROWS = BLOCK // PIECES
DEEP = DEPTH // PIECES
PAIR = 2 * BLOCK


def place(a, b, y, z, c):
    return (b * 4 + z, a * 8 + y * 2 + c)


def kernel(
    x_ref,
    outbuf,
    rbuf,
    cbuf,
    csend,
    tbuf,
    rhi,
    rlo,
    chi,
    clo,
    send,
    t_recv,
    tr_recv,
    x_recv,
    b_recv,
    y1_recv,
    y2_recv,
    z1_recv,
    z2_recv,
    d_recv,
):
    row, col = lax.axis_index("row"), lax.axis_index("col")
    b, z = row // 4, row % 4
    a, y, c = col // 8, (col // 2) % 4, col % 2
    up, down = 1, 3

    twin = place(a, b, y, z, 1 - c)
    across = place(1 - a, b, y, z, c)
    beside = place(a, 1 - b, y, z, c)
    y_dev = {d: place(a, b, (y + d) % 4, z, c) for d in (up, down)}
    z_dev = {d: place(a, b, y, (z + d) % 4, c) for d in (up, down)}
    t_to = place(b, 1 - c, z, (2 * z + 4 - y) % 4, a)
    t_from = place(c, a, (2 * y + 4 - z) % 4, y, 1 - b)
    off = (y + 4 - z) % 4
    turns = (1, 3)

    def corner_from(e):
        return place(c, a, (y + 6 - e) % 4, (z + 4 - e) % 4, 1 - b)

    def corner_to(e):
        return place(a, b, (y + 4 - e) % 4, (z + 6 - e) % 4, c)

    def side_from(d):
        return place(c, a, y, (y + 4 - d) % 4, 1 - b)

    def side_to(d):
        return place(a, b, (y + 4 - d) % 4, z, c)

    def r_pair(flip, dy):
        return (a + flip) % 2 * 4 + (y + dy) % 4

    def c_pair(dz):
        return (2 * y + 8 - z - dz) % 4

    barrier = pltpu.get_barrier_semaphore()

    def here(*devices):
        for device in devices:
            pl.semaphore_signal(barrier, inc=1, device_id=device, device_id_type=MESH)

    here(twin, across, beside, y_dev[up], y_dev[down], z_dev[up], z_dev[down], t_from)

    @pl.when(off % 2 == 1)
    def _():
        here(place(a, b, (y + off) % 4, z, c))

    @pl.when(off == 2)
    def _():
        here(*(side_from(d) for d in turns))
        here(*(place(a, b, (y + e) % 4, (y + e) % 4, c) for e in turns))

    @pl.when(off == 0)
    def _():
        here(*(corner_from(e) for e in turns))

    own = r_pair(0, 0) * 2 + c

    def normalise(i, _):
        x = x_ref[pl.ds(i * 8, 8)]
        variance = jnp.sum(x * x, axis=1, keepdims=True)
        scaled = (x * (1.0 / jnp.sqrt(variance))).reshape(8 * FACTORS, BLOCK)
        at = pl.ds(pl.multiple_of(i * 8 * FACTORS, 8 * FACTORS), 8 * FACTORS)
        csend[at, :] = scaled
        rbuf[own, :, at] = scaled.T
        return 0

    lax.fori_loop(0, SAMPLES // 8, normalise, 0)
    odd = off % 2
    pl.semaphore_wait(barrier, 8 + odd + (1 - odd) * (2 + 2 * (off // 2)))

    def go(src, dst, sem, recv, device):
        pltpu.make_async_remote_copy(
            src_ref=src, dst_ref=dst, send_sem=send.at[sem], recv_sem=recv, device_id=device, device_id_type=MESH
        ).start()

    def r_piece(block, i):
        return rbuf.at[block, pl.ds(i * ROWS, ROWS), :]

    def c_piece(block, i):
        return cbuf.at[block, pl.ds(i * DEEP, DEEP), :]

    def arrived(ref, sem):
        pltpu.make_async_copy(ref, ref, sem).wait()

    def r_go(block, i, sem, recv, device):
        go(r_piece(block, i), r_piece(block, i), sem, recv, device)

    def c_go(block, i, sem, recv, device):
        go(c_piece(block, i), c_piece(block, i), sem, recv, device)

    S_T, S_X, S_B, S_YU, S_YD, S_ZU, S_ZD, S_D, S_TR = range(9)

    def hand_over(flip, dy):
        pair = r_pair(flip, dy)
        go(rbuf.at[pair * 2 + c], rbuf.at[pair * 2 + c], S_D, d_recv.at[pair], twin)

    def y_first(k, i):
        block = r_pair(k, 0) * 2 + c
        r_go(block, i, S_YU, y1_recv.at[0, k, i], y_dev[up])
        r_go(block, i, S_YD, y1_recv.at[1, k, i], y_dev[down])

    def z_first(k, block, i):
        c_go(block, i, S_ZU, z1_recv.at[0, k, i], z_dev[up])
        c_go(block, i, S_ZD, z1_recv.at[1, k, i], z_dev[down])

    def each(n, body):
        def step(i, _):
            body(i)
            return 0

        lax.fori_loop(0, n, step, 0)

    t_slot = y * 2 + c
    own_t = c_pair(0) * 2 + 1 - b
    own_b = c_pair(0) * 2 + b

    def transposed(i):
        src = csend.at[pl.ds(i * DEEP, DEEP), :]
        aside = (off % 2) * (i % 4 // 3) + (off // 2) * (1 - off % 2)
        f, slot = i % 2, i // 2

        @pl.when(aside == 0)
        def _():
            go(src, c_piece(t_slot, i), S_T, t_recv.at[i], t_to)

        @pl.when(aside * (off % 2) == 1)
        def _():
            g = off // 2
            go(src, tbuf.at[g, i // 4], S_T, tr_recv.at[g, i // 4], place(b, 1 - c, y, (z + 4 - off) % 4, a))

        @pl.when(aside * (1 - off % 2) == 1)
        def _():
            w = (z + 1 + 2 * f) % 4
            go(src, tbuf.at[f, slot], S_T, tr_recv.at[f, slot], place(b, 1 - c, w, w, a))

    def start(i):
        @pl.when(i < 3)
        def _():
            y_first(0, i)

    def pass_corner(i):
        f, slot = i % 2, i // 2

        @pl.when(off == 0)
        def _():
            e = 1 + 2 * f
            arrived(tbuf.at[f, slot], tr_recv.at[f, slot])
            at = (y + 6 - e) % 4 * 2 + 1 - b
            go(tbuf.at[f, slot], c_piece(at, i), S_TR, t_recv.at[i], corner_to(e))

    def pass_side(i):
        f, slot = i % 2, i // 2

        @pl.when((off // 2) * (1 - off % 2) * (1 - i // 4) == 1)
        def _():
            arrived(tbuf.at[f, slot], tr_recv.at[f, slot])
            p = 4 * slot + 3
            go(tbuf.at[f, slot], c_piece(y * 2 + 1 - b, p), S_TR, t_recv.at[p], side_to(1 + 2 * f))

    each(PIECES, transposed)
    each(PIECES, start)
    hand_over(0, 0)

    def split_rows(pair, half):
        def body(i):
            at = pl.ds(pl.multiple_of(i * 16, 16), 16)
            v = rbuf[pair * 2 + half, at, :]
            hi = v.astype(jnp.bfloat16)
            to = pl.ds(pl.multiple_of(pair * PAIR + half * BLOCK + i * 16, 16), 16)
            rhi[to, :] = hi
            rlo[to, :] = (v - hi.astype(jnp.float32)).astype(jnp.bfloat16)

        each(BLOCK // 16, body)

    def ready_rows(flip, dy):
        pair = r_pair(flip, dy)
        arrived(rbuf.at[pair * 2 + 1 - c], d_recv.at[pair])
        split_rows(pair, 0)
        split_rows(pair, 1)

    def blocks_of(slot):
        beyond = (slot + 1) // 2
        which = (slot + b) % 2
        left = (1 - beyond) * (c_pair(0) * 2) + beyond * (c_pair(up) * 2 + which)
        right = (1 - beyond) * (c_pair(0) * 2 + 1) + beyond * (c_pair(down) * 2 + which)
        return left, right

    def split_columns(species, slot, side, i):
        at = pl.ds(pl.multiple_of(i * DEEP, DEEP), DEEP)
        v = cbuf[species, at, :]
        hi = v.astype(jnp.bfloat16)
        to = slice(side * BLOCK, (side + 1) * BLOCK)
        chi[slot, at, to] = hi
        clo[slot, at, to] = (v - hi.astype(jnp.float32)).astype(jnp.bfloat16)

    def ready_columns(slot):
        for side, species in enumerate(blocks_of(slot)):
            each(PIECES, lambda i: split_columns(species, slot, side, i))

    def dot(left, right):
        return jnp.dot(left, right, preferred_element_type=jnp.float32)

    def block(start, n, slot, columns_of):
        rows = pl.ds(pl.multiple_of(start * PAIR, PAIR), n * PAIR)
        right = chi[slot]
        total = dot(rhi[rows, :], right) + dot(rhi[rows, :], clo[slot]) + dot(rlo[rows, :], right)
        total = total * (1.0 / SAMPLES)
        for side, species in enumerate(columns_of):
            columns = pl.ds(pl.multiple_of(species * BLOCK, BLOCK), BLOCK)
            outbuf[rows, columns] = total[:, side * BLOCK : (side + 1) * BLOCK]

    def tile(p, slot):
        block(p, 1, slot, blocks_of(slot))

    def turn(m):
        return m + m // 2 - 2 * (m // 3)

    ready_rows(0, 0)

    def y_second(k, half):
        even, odd = 2 * half, 2 * half + 1
        below, above = r_pair(k, down) * 2 + c, r_pair(k, up) * 2 + c
        for i in (even, odd):
            arrived(r_piece(below, i), y1_recv.at[0, k, i])
            arrived(r_piece(above, i), y1_recv.at[1, k, i])
        r_go(below, even, S_YU, y2_recv.at[0, k, half], y_dev[up])
        r_go(above, odd, S_YD, y2_recv.at[1, k, half], y_dev[down])

    def z_second(k, half):
        even, odd = 2 * half, 2 * half + 1
        s = (1 - b + k) % 2
        below, above = c_pair(down) * 2 + s, c_pair(up) * 2 + s
        for i in (even, odd):
            arrived(c_piece(below, i), z1_recv.at[0, k, i])
            arrived(c_piece(above, i), z1_recv.at[1, k, i])
        c_go(below, even, S_ZU, z2_recv.at[0, k, half], z_dev[up])
        c_go(above, odd, S_ZD, z2_recv.at[1, k, half], z_dev[down])

    def early(i):
        @pl.when((off // 2) * (1 - off % 2) * (i % 2) == 1)
        def _():
            z_second(0, i // 2)

        pass_side(i)
        arrived(c_piece(own_t, i), t_recv.at[i])
        z_first(0, own_t, i)
        c_go(own_t, i, S_B, b_recv.at[i], beside)
        r_go(own, i, S_X, x_recv.at[i], across)
        pass_corner(i)

        @pl.when(i < PIECES - 3)
        def _():
            y_first(0, i + 3)

        @pl.when(i >= PIECES // 2)
        def _():
            y_second(0, i - PIECES // 2)

    each(PIECES, early)

    def middle(i):
        arrived(r_piece(r_pair(1, 0) * 2 + c, i), x_recv.at[i])
        y_first(1, i)

        @pl.when((i // 4) * (1 - (off // 2) * (1 - off % 2)) == 1)
        def _():
            z_second(0, i - PIECES // 2)

        arrived(c_piece(own_b, i), b_recv.at[i])
        z_first(1, own_b, i)

    each(PIECES, middle)
    hand_over(0, up)
    hand_over(0, down)
    hand_over(1, 0)
    ready_columns(0)
    ready_columns(1)

    def y_last(k):
        far = r_pair(k, 2) * 2 + c
        for half in range(PIECES // 2):
            arrived(r_piece(far, 2 * half), y2_recv.at[0, k, half])
            arrived(r_piece(far, 2 * half + 1), y2_recv.at[1, k, half])
        hand_over(k, 2)

    for half in range(PIECES // 2):
        y_second(1, half)
        flip, dy = ((0, 0), (0, up), (0, down), (1, 0))[half]
        if half:
            ready_rows(flip, dy)
        each(2, lambda slot: tile(r_pair(flip, dy), slot))
    hand_over(1, up)
    hand_over(1, down)
    for half in range(PIECES // 2):
        if half == 3:
            y_last(1)
        z_second(1, half)
        if half == 0:
            y_last(0)
        else:
            flip, dy = ((1, up), (1, down), (0, 2))[half - 1]
            ready_rows(flip, dy)
            each(2, lambda slot: tile(r_pair(flip, dy), slot))
    ready_columns(2)
    last = r_pair(1, 2)
    each(3, lambda m: block((last // 2 + 1 + m) % 4 * 2, 2, 2, blocks_of(2)))
    ready_rows(1, 2)
    block(last // 2 * 2, 2, 2, blocks_of(2))
    each(2, lambda slot: tile(last, slot))

    far = (c_pair(2) * 2, c_pair(2) * 2 + 1)
    for k in range(2):
        species = c_pair(2) * 2 + (1 - b + k) % 2
        for half in range(PIECES // 2):
            arrived(c_piece(species, 2 * half), z2_recv.at[0, k, half])
            arrived(c_piece(species, 2 * half + 1), z2_recv.at[1, k, half])
    for side in range(2):
        each(PIECES, lambda i: split_columns(far[side], 0, side, i))
    each(4, lambda m: block(m * 2, 2, 0, far))

    for sem, blocks in ((S_T, 1), (S_X, 1), (S_B, 1), (S_YU, 3), (S_YD, 3), (S_ZU, 3), (S_ZD, 3), (S_D, 8)):
        arrived(rbuf.at[pl.ds(0, blocks)], send.at[sem])

    @pl.when(off == 0)
    def _():
        arrived(rbuf.at[0], send.at[S_TR])

    @pl.when(off == 2)
    def _():
        arrived(rbuf.at[0, pl.ds(0, BLOCK // 2), :], send.at[S_TR])


def write_out(held, out_ref, sem):
    for i in range(8):
        rows = pl.ds(i * PAIR, PAIR)
        pltpu.make_async_copy(held.at[rows], out_ref.at[rows], sem).start()
    pltpu.make_async_copy(held, out_ref, sem).wait()


def local(loadings):
    dma = pltpu.SemaphoreType.DMA
    held = pl.pallas_call(
        kernel,
        out_shape=pltpu.VMEM((16 * BLOCK, 8 * BLOCK), jnp.float32),
        in_specs=[pl.BlockSpec(memory_space=pltpu.VMEM)],
        out_specs=pl.BlockSpec(memory_space=pltpu.VMEM),
        scratch_shapes=[
            pltpu.VMEM((16, BLOCK, DEPTH), jnp.float32),
            pltpu.VMEM((8, DEPTH, BLOCK), jnp.float32),
            pltpu.VMEM((DEPTH, BLOCK), jnp.float32),
            pltpu.VMEM((2, PIECES // 2, DEEP, BLOCK), jnp.float32),
            pltpu.VMEM((8 * PAIR, DEPTH), jnp.bfloat16),
            pltpu.VMEM((8 * PAIR, DEPTH), jnp.bfloat16),
            pltpu.VMEM((3, DEPTH, PAIR), jnp.bfloat16),
            pltpu.VMEM((3, DEPTH, PAIR), jnp.bfloat16),
            dma((9,)),
            dma((PIECES,)),
            dma((2, PIECES // 2)),
            dma((PIECES,)),
            dma((PIECES,)),
            dma((2, 2, PIECES)),
            dma((2, 2, PIECES // 2)),
            dma((2, 2, PIECES)),
            dma((2, 2, PIECES // 2)),
            dma((8,)),
        ],
        compiler_params=pltpu.CompilerParams(
            collective_id=0, has_side_effects=True, vmem_limit_bytes=54 * 1024 * 1024
        ),
    )(loadings)
    return pl.pallas_call(
        write_out,
        out_shape=jax.ShapeDtypeStruct(held.shape, held.dtype),
        in_specs=[pl.BlockSpec(memory_space=pltpu.VMEM)],
        out_specs=pl.BlockSpec(memory_space=pl.ANY),
        scratch_shapes=[dma],
        compiler_params=pltpu.CompilerParams(vmem_limit_bytes=1024 * 1024),
    )(held)


def solution(mesh):
    placed = (P(None, None, ("row", "col")),)
    return jax.shard_map(local, mesh=mesh, in_specs=placed, out_specs=P("row", "col"), check_vma=False)
```
